32 devices in a mesh: layer: 8 (over z, x), split: 4 (over y, core).
Axes of the slice: x: 2, y: 2, z: 4, core: 2. Of those that a mesh axis runs over, the one named last changes fastest.
Arguments:
- right_side: float32 [32, 512, 128], P('layer', 'split'), may hold values from -6 to 6
- diagonal: float32 [32, 512, 128], P('layer', 'split'), may hold values from 0.1 to 1
- inverses: float32 [32, 512, 512], P('layer', None, 'split'), may hold values from -1 to 1, as said below
Outputs:
- solution_field: float32 [32, 512, 128], P('layer', 'split')
- residual: float32 [32, 512, 128], P('layer', 'split')
The draws below stay inside these ranges and needn't reach their ends.
Inputs may be any that keep to these rules, and one draw needn't show every extreme that they name: `inverses`: each plane's inverse is a diagonal matrix with entries between 0.5 and 1 plus a dense coupling with zero diagonal and spectral norm below 0.2.
All inputs are finite; a program needn't handle non-finite values.
Results may differ from the reference program's by a relative error of at most 0.0003.
Values sent between devices are 32-bit elements; how exact they have to be, the bound alone decides.
A program may use at most 64 MiB of HBM per device.

```python
import jax
import jax.numpy as jnp
from jax import lax

NX = 512
NY = 128
SHEET_TOTAL = 32


def draw_inverses(key, part):
    speed_seed, sheet_seed, pulse_seed, linkage_seed = jax.random.split(jax.random.fold_in(key, 11), 4)
    low_rate = jnp.log(0.5 / SHEET_TOTAL)
    high_rate = jnp.log(1.0 / 30.0)
    base_rate = jnp.exp(jax.random.uniform(speed_seed, (1, NX), jnp.float32, low_rate, high_rate))
    plane_factor = jax.random.uniform(sheet_seed, (SHEET_TOTAL, 1), jnp.float32, 0.6, 1.4)
    retained_share = jnp.exp(-base_rate * plane_factor)
    pulse_batches = jax.random.uniform(pulse_seed, (SHEET_TOTAL, 1), jnp.float32) < 6.0 / SHEET_TOTAL
    retained_share = jnp.where(pulse_batches, 0.6 * retained_share, retained_share)
    coupling = jax.random.normal(linkage_seed, (SHEET_TOTAL, NX, NX), jnp.float32) * (0.05 / jnp.sqrt(1.0 * NX))
    identity = jnp.eye(NX, dtype=jnp.float32)[None, :, :]
    coupling = coupling * (1.0 - identity)
    return coupling + retained_share[:, :, None] * identity


def block_scale(own_key, extent, shards, smallest, high):
    def one(axis_at, parts):
        steps = jax.random.uniform(jax.random.fold_in(jax.random.fold_in(own_key, 6), axis_at), (parts,), jnp.float32, smallest / len(shards), high / len(shards))
        return jnp.repeat(jnp.exp(steps), extent[axis_at] // parts).reshape((-1,) + (1,) * (len(extent) - axis_at - 1))

    level = one(*shards[0])
    for cut in shards[1:]:
        level = level * one(*cut)
    return level


def gaussian(stream_key, dims, deviation, limit, shards=(), kind=jnp.bfloat16):
    gain = block_scale(stream_key, dims, shards, -0.22, 0.18) if shards else 1.0
    values = jax.random.normal(stream_key, dims, jnp.float32) * deviation * gain
    return jnp.minimum(jnp.maximum(values, -limit), limit).astype(kind)


def setup_inputs(seed: int = 0) -> dict:
    key_list = jax.random.split(jax.random.key(seed), 4)
    right_side = gaussian(key_list[0], (SHEET_TOTAL, NX, NY), 1.0, 6.0, ((0, 8), (1, 4)), jnp.float32)
    diagonal = jnp.clip(0.1 + 0.9 * jax.random.uniform(key_list[1], (SHEET_TOTAL, NX, NY), jnp.float32) ** block_scale(key_list[1], (SHEET_TOTAL, NX, NY), ((0, 8), (1, 4)), -0.2, 0.2), 0.1, 1.0)
    inverses = draw_inverses(jax.random.fold_in(key_list[3], 71), 0)
    return {"right_side": right_side, "diagonal": diagonal, "inverses": inverses}


def stencil(values, diagonal):
    padded = jnp.pad(values, 1)
    beside = padded[2:, 1:-1, 1:-1] + padded[:-2, 1:-1, 1:-1]
    beside = beside + padded[1:-1, 2:, 1:-1] + padded[1:-1, :-2, 1:-1]
    beside = beside + padded[1:-1, 1:-1, 2:] + padded[1:-1, 1:-1, :-2]
    return (6.0 + diagonal) * values - beside


def reference(right_side, diagonal, inverses):
    highest = lax.Precision.HIGHEST

    def down_plane(carried, inputs):
        matrix, source = inputs
        carried = jnp.dot(matrix, source + carried, precision=highest)
        return carried, carried

    start = jnp.zeros((NX, NY), jnp.float32)
    _, lower_sweep = lax.scan(down_plane, start, (inverses, right_side))

    def up_plane(carried, inputs):
        matrix, below = inputs
        summed = below + jnp.dot(matrix, carried, precision=highest)
        return summed, summed

    _, direction = lax.scan(up_plane, start, (inverses, lower_sweep), reverse=True)
    image = stencil(direction, diagonal)
    step_alpha = jnp.sum(right_side * right_side) / jnp.sum(right_side * image)
    middle = right_side - step_alpha * image
    tangent = stencil(middle, diagonal)
    step_omega = jnp.sum(tangent * middle) / jnp.sum(tangent * tangent)
    return step_alpha * direction + step_omega * middle, middle - step_omega * tangent
```

```python
import functools

import jax
import jax.numpy as jnp
from jax import lax
from jax.experimental import pallas as pl
from jax.experimental.pallas import tpu as pltpu
from jax.sharding import PartitionSpec as P

MESH = pl.DeviceIdType.MESH
F32, BF16 = jnp.float32, jnp.bfloat16


def halves(a):
    hi = a.astype(BF16)
    return hi, (a - hi.astype(F32)).astype(BF16)


def product(a_hi, a_lo, b_hi, b_lo, axis):
    dims = (((1,), (axis,)), ((), ()))

    def one(a, b):
        return lax.dot_general(a, b, dims, preferred_element_type=F32)

    return one(a_hi, b_hi) + (one(a_lo, b_hi) + one(a_hi, b_lo))


def sweep_kernel(
    depth, parts, rs_ref, inv_ref, out_ref,
    mf, mhi, mlo, whi, wlo, uhi, ulo, loc, base, rsend, rrecv, vin, vout, din, dout, dsend, drecv,
    own_sem, gs_sem, gr_sem, as_sem, ar_sem, bs_sem, br_sem, vs_sem, vr_sem, ds_sem, dr_sem,
):
    planes, nx, xb = inv_ref.shape
    ny = rs_ref.shape[2]
    yb = ny // parts
    chunks = vin.shape[0]
    cb = yb // chunks
    l, s = lax.axis_index("layer"), lax.axis_index("split")
    bits = [1 << i for i in range(parts.bit_length() - 1)]

    barrier = pltpu.get_barrier_semaphore()
    for r in range(1, parts):
        pl.semaphore_signal(barrier, inc=1, device_id=(l, s ^ r), device_id_type=MESH)
    pl.semaphore_signal(barrier, inc=1, device_id=(lax.rem(l + 1, depth), s), device_id_type=MESH)
    pl.semaphore_signal(barrier, inc=1, device_id=(lax.rem(l + depth - 1, depth), s), device_id_type=MESH)

    def own_copy(k):
        return pltpu.make_async_copy(inv_ref.at[k], mf.at[k, s], own_sem.at[k])

    for k in range(planes):
        own_copy(k).start()
    for k in range(planes):
        turned = jnp.transpose(rs_ref[k])
        for r in range(parts):
            rsend[r, k] = turned[r * yb:(r + 1) * yb]
    pl.semaphore_wait(barrier, parts + 1)

    def regroup(src, dst, ssem, rsem, r):
        return pltpu.make_async_remote_copy(
            src_ref=src.at[s ^ r], dst_ref=dst.at[s], send_sem=ssem.at[r], recv_sem=rsem.at[r],
            device_id=(l, s ^ r), device_id_type=MESH)

    def regroup_in(src, dst, ssem, rsem, r):
        return pltpu.make_async_remote_copy(
            src_ref=src.at[s ^ r], dst_ref=dst.at[s ^ r], send_sem=ssem.at[r], recv_sem=rsem.at[r],
            device_id=(l, s ^ r), device_id_type=MESH)

    def shift(k, r, b):
        src = inv_ref.at[k] if r == 0 else mf.at[k, s ^ r]
        return pltpu.make_async_remote_copy(
            src_ref=src, dst_ref=mf.at[k, s ^ r], send_sem=gs_sem.at[k, r ^ b], recv_sem=gr_sem.at[k, r ^ b],
            device_id=(l, s ^ b), device_id_type=MESH)

    def arrived(k, r):
        return pltpu.make_async_remote_copy(
            src_ref=mf.at[k, s ^ r], dst_ref=mf.at[k, s ^ r], send_sem=gs_sem.at[k, r], recv_sem=gr_sem.at[k, r],
            device_id=(l, s ^ 1), device_id_type=MESH)

    for r in range(1, parts):
        regroup(rsend, rrecv, as_sem, ar_sem, r).start()
    for k in range(planes):
        for b in reversed(bits):
            shift(k, 0, b).start()
    rrecv[s] = rsend[s]
    for r in range(1, parts):
        regroup_in(rsend, rrecv, as_sem, ar_sem, r).wait_recv()

    def fetch(k):
        for r in range(1, parts):
            arrived(k, r).wait_recv()
            for b in bits:
                if b < (r & -r):
                    shift(k, r, b).start()
        own_copy(k).wait()
        for j in range(parts):
            hi, lo = halves(mf[k, j])
            mhi[k, :, j * xb:(j + 1) * xb] = hi
            mlo[k, :, j * xb:(j + 1) * xb] = lo

    def source(k):
        return jnp.concatenate([rrecv[j, k] for j in range(parts)], axis=1)

    half = nx // 2

    fetch(0)
    for j in range(parts):
        hi, lo = halves(jnp.transpose(mf[0, j]))
        whi[0, j * xb:(j + 1) * xb] = hi
        wlo[0, j * xb:(j + 1) * xb] = lo
    loc[0] = product(*halves(source(0)), mhi[0], mlo[0], 1)

    @pl.loop(1, planes)
    def _(k):
        fetch(k)
        loc[k] = product(*halves(source(k) + loc[k - 1]), mhi[k], mlo[k], 1)
        for t in range(2):
            rows = slice(t * half, (t + 1) * half)
            hi, lo = halves(product(whi[k - 1, rows], wlo[k - 1, rows], mhi[k], mlo[k], 1))
            whi[k, rows] = hi
            wlo[k, rows] = lo

    last = planes - 1

    def hop(src, dst, ssem, rsem, c, step):
        return pltpu.make_async_remote_copy(
            src_ref=src.at[c], dst_ref=dst.at[c], send_sem=ssem.at[c], recv_sem=rsem.at[c],
            device_id=(lax.rem(l + step + depth, depth), s), device_id_type=MESH)

    def down_chain():
        for c in range(chunks):
            rows = slice(c * cb, (c + 1) * cb)

            @pl.when(l > 0)
            def _():
                hop(vout, vin, vs_sem, vr_sem, c, 1).wait_recv()

            @pl.when(l == 0)
            def _():
                vin[c] = jnp.zeros_like(vin[c])

            vout[c] = loc[last, rows] + product(*halves(vin[c]), whi[last], wlo[last], 0)

            @pl.when(l < depth - 1)
            def _():
                hop(vout, vin, vs_sem, vr_sem, c, 1).start()

    def compose():
        for j in range(parts):
            hi, lo = halves(jnp.transpose(mf[last, j]))
            uhi[last, j * xb:(j + 1) * xb] = hi
            ulo[last, j * xb:(j + 1) * xb] = lo

        @pl.loop(0, last)
        def _(i):
            k = last - 1 - i
            loc[k] = loc[k] + product(*halves(loc[k + 1]), mhi[k], mlo[k], 1)
            for t in range(2):
                rows = slice(t * half, (t + 1) * half)
                hi, lo = halves(product(uhi[k + 1, rows], ulo[k + 1, rows], mhi[k], mlo[k], 1))
                uhi[k, rows] = hi
                ulo[k, rows] = lo
                own = whi[k, rows].astype(F32) + wlo[k, rows].astype(F32)
                hi, lo = halves(own + product(whi[k + 1, rows], wlo[k + 1, rows], mhi[k], mlo[k], 1))
                whi[k, rows] = hi
                wlo[k, rows] = lo

    early = lax.convert_element_type(l < depth // 2, jnp.int32)

    @pl.loop(0, 2)
    def _(turn):
        @pl.when(turn != early)
        def _():
            down_chain()

        @pl.when(turn == early)
        def _():
            compose()

    entering = jnp.concatenate([vin[c] for c in range(chunks)], axis=0)
    entering = halves(entering)

    @pl.loop(0, planes)
    def _(k):
        base[k] = loc[k] + product(*entering, whi[k], wlo[k], 0)

    for c in range(chunks):
        rows = slice(c * cb, (c + 1) * cb)

        @pl.when(l < depth - 1)
        def _():
            hop(dout, din, ds_sem, dr_sem, c, -1).wait_recv()

        @pl.when(l == depth - 1)
        def _():
            din[c] = jnp.zeros_like(din[c])

        dout[c] = base[0, rows] + product(*halves(din[c]), uhi[0], ulo[0], 0)

        @pl.when(l > 0)
        def _():
            hop(dout, din, ds_sem, dr_sem, c, -1).start()

    entering = halves(jnp.concatenate([din[c] for c in range(chunks)], axis=0))

    @pl.loop(0, planes)
    def _(k):
        swept = base[k] + product(*entering, uhi[k], ulo[k], 0)
        for j in range(parts):
            dsend[j, k] = swept[:, j * xb:(j + 1) * xb]

    for r in range(1, parts):
        regroup(dsend, drecv, bs_sem, br_sem, r).start()
    drecv[s] = dsend[s]
    for r in range(1, parts):
        regroup_in(dsend, drecv, bs_sem, br_sem, r).wait_recv()
    for k in range(planes):
        out_ref[k] = jnp.transpose(jnp.concatenate([drecv[j, k] for j in range(parts)], axis=0))

    for r in range(1, parts):
        regroup(rsend, rrecv, as_sem, ar_sem, r).wait_send()
        regroup(dsend, drecv, bs_sem, br_sem, r).wait_send()
    for k in range(planes):
        for r in range(1, parts):
            arrived(k, r).wait_send()
    for c in range(chunks):
        @pl.when(l < depth - 1)
        def _():
            hop(vout, vin, vs_sem, vr_sem, c, 1).wait_send()

        @pl.when(l > 0)
        def _():
            hop(dout, din, ds_sem, dr_sem, c, -1).wait_send()


def sweep(right_side, inverses):
    depth, parts = lax.axis_size("layer"), lax.axis_size("split")
    planes, nx, xb = inverses.shape
    ny = right_side.shape[2]
    yb = ny // parts
    chunks = 2 if yb % 16 == 0 else 1
    square = pltpu.VMEM((planes, nx, nx), BF16)
    lines = pltpu.VMEM((planes, yb, nx), F32)
    pieces = pltpu.VMEM((parts, planes, yb, xb), F32)
    carry = pltpu.VMEM((chunks, yb // chunks, nx), F32)
    dma = pltpu.SemaphoreType.DMA
    return pl.pallas_call(
        functools.partial(sweep_kernel, depth, parts),
        out_shape=jax.ShapeDtypeStruct(right_side.shape, F32),
        in_specs=[pl.BlockSpec(memory_space=pltpu.VMEM)] * 2,
        out_specs=pl.BlockSpec(memory_space=pltpu.VMEM),
        scratch_shapes=[
            pltpu.VMEM((planes, parts, nx, xb), F32),
            square, square, square, square, square, square,
            lines, lines, pieces, pieces, carry, carry, carry, carry, pieces, pieces,
            dma((planes,)), dma((planes, parts)), dma((planes, parts)),
            dma((parts,)), dma((parts,)), dma((parts,)), dma((parts,)),
            dma((chunks,)), dma((chunks,)), dma((chunks,)), dma((chunks,)),
        ],
        compiler_params=pltpu.CompilerParams(
            collective_id=0, has_side_effects=True, vmem_limit_bytes=60 * 1024 * 1024),
    )(right_side, inverses)


def with_halo(x, sides, width):
    for axis, dim in sides:
        size, length = (lax.axis_size(axis), x.shape[dim])
        up = [(i, (i + 1) % size) for i in range(size - 1)]
        down = [(j, i) for i, j in up]
        last = lax.slice_in_dim(x, length - width, length, axis=dim)
        first = lax.slice_in_dim(x, 0, width, axis=dim)
        before = lax.ppermute(last, axis, up)
        after = lax.ppermute(first, axis, down)
        x = jnp.concatenate([before, x, after], axis=dim)
    return x


def stencil(values, diagonal):
    padded = with_halo(values, (("layer", 0), ("split", 1)), 1)
    beside = padded[2:, 1:-1, :] + padded[:-2, 1:-1, :]
    beside = beside + padded[1:-1, 2:, :] + padded[1:-1, :-2, :]
    centre_part = padded[1:-1, 1:-1, :]
    y_upper = jnp.pad(centre_part[:, :, 1:], ((0, 0), (0, 0), (0, 1)))
    y_lower = jnp.pad(centre_part[:, :, :-1], ((0, 0), (0, 0), (1, 0)))
    return (6.0 + diagonal) * values - beside - y_upper - y_lower


def per_device(right_side, diagonal, inverses):
    applied_rhs = stencil(right_side, diagonal)
    direction = sweep(right_side, inverses)
    image = stencil(direction, diagonal)
    applied_image = stencil(image, diagonal)
    sums_all = lax.psum(
        (
            jnp.sum(right_side * right_side),
            jnp.sum(right_side * image),
            jnp.sum(applied_rhs * right_side),
            jnp.sum(applied_rhs * image),
            jnp.sum(applied_image * right_side),
            jnp.sum(applied_image * image),
            jnp.sum(applied_rhs * applied_rhs),
            jnp.sum(applied_rhs * applied_image),
            jnp.sum(applied_image * applied_image),
        ),
        ("layer", "split"),
    )
    (
        norm_sq,
        curv_sum,
        rhs_rhs,
        rhs_image,
        image_rhs,
        image_image,
        arhs_arhs,
        arhs_aimage,
        aimage_aimage,
    ) = sums_all
    step_alpha = norm_sq / curv_sum
    middle = right_side - step_alpha * image
    tangent = applied_rhs - step_alpha * applied_image
    cross_sum = (
        rhs_rhs - step_alpha * (rhs_image + image_rhs) + step_alpha * step_alpha * image_image
    )
    self_sum = arhs_arhs - 2.0 * step_alpha * arhs_aimage + step_alpha * step_alpha * aimage_aimage
    step_omega = cross_sum / self_sum
    solution_field = step_alpha * direction + step_omega * middle
    residual = middle - step_omega * tangent
    return (solution_field, residual)


def solution(mesh):
    placed = (P("layer", "split", None), P("layer", "split", None), P("layer", None, "split"))
    return jax.shard_map(
        per_device,
        mesh=mesh,
        in_specs=placed,
        out_specs=(P("layer", "split", None), P("layer", "split", None)),
        check_vma=False,
    )
```

```python
import functools

import jax
import jax.numpy as jnp
from jax import lax
from jax.experimental import pallas as pl
from jax.experimental.pallas import tpu as pltpu
from jax.sharding import PartitionSpec as P

MESH = pl.DeviceIdType.MESH
F32, BF16 = jnp.float32, jnp.bfloat16


def halves(a):
    hi = a.astype(BF16)
    return hi, (a - hi.astype(F32)).astype(BF16)


def product(a_hi, a_lo, b_hi, b_lo, axis):
    dims = (((1,), (axis,)), ((), ()))

    def one(a, b):
        return lax.dot_general(a, b, dims, preferred_element_type=F32)

    return one(a_hi, b_hi) + (one(a_lo, b_hi) + one(a_hi, b_lo))


def sweep_kernel(
    depth, parts, rs_ref, diag_ref, inv_ref, sol_ref, res_ref,
    mf, mhi, mlo, whi, wlo, uhi, ulo, loc, base, rsend, rrecv, vin, vout, din, dout, dsend, drecv,
    arhs, dirn, img, aimg, zh, xh, xs, srow, sall, trow, tall,
    hs_sem, hr_sem, ls_sem, lr_sem, ts_sem, tr_sem,
    own_sem, gs_sem, gr_sem, as_sem, ar_sem, bs_sem, br_sem, vs_sem, vr_sem, ds_sem, dr_sem,
):
    planes, nx, xb = inv_ref.shape
    ny = rs_ref.shape[2]
    yb = ny // parts
    chunks = vin.shape[0]
    cb = yb // chunks
    l, s = lax.axis_index("layer"), lax.axis_index("split")
    bits = [1 << i for i in range(parts.bit_length() - 1)]

    last = planes - 1
    row_at = lax.broadcasted_iota(jnp.int32, (xb, ny), 0)
    col_at = lax.broadcasted_iota(jnp.int32, (xb, ny), 1)

    def stage_lines(h, ref):
        for k in range(planes):
            xs[h, 0, k:k + 1] = ref[k, 0:1]
            xs[h, 1, k:k + 1] = ref[k, xb - 1:xb]

    def halo_copies(h, ref):
        def zcopy(side, slot):
            return pltpu.make_async_remote_copy(
                src_ref=ref.at[0 if side == 0 else last], dst_ref=zh.at[h, slot], send_sem=hs_sem.at[h, side],
                recv_sem=hr_sem.at[h, slot],
                device_id=(lax.rem(l + 2 * side - 1 + depth, depth), s), device_id_type=MESH)

        def xcopy(side, slot):
            return pltpu.make_async_remote_copy(
                src_ref=xs.at[h, side], dst_ref=xh.at[h, slot], send_sem=hs_sem.at[h, 2 + side],
                recv_sem=hr_sem.at[h, 2 + slot],
                device_id=(l, lax.rem(s + 2 * side - 1 + parts, parts)), device_id_type=MESH)

        out = []
        for side in range(2):
            zhas = l > 0 if side == 0 else l < depth - 1
            xhas = s > 0 if side == 0 else s < parts - 1
            for has, copy, slot in ((zhas, zcopy, zh), (xhas, xcopy, xh)):
                out.append((
                    has, functools.partial(copy, side, 1 - side), functools.partial(copy, side, side),
                    slot.at[h, side]))
        return out

    def halo_start(h, ref):
        for has, copy, _, _ in halo_copies(h, ref):
            @pl.when(has)
            def _():
                copy().start()

    def halo_wait(h, ref):
        for has, _, back, slot in halo_copies(h, ref):
            @pl.when(has)
            def _():
                back().wait_recv()

            @pl.when(jnp.logical_not(has))
            def _():
                slot[...] = jnp.zeros_like(slot[...])

    def halo_finish(h, ref):
        for has, copy, _, _ in halo_copies(h, ref):
            @pl.when(has)
            def _():
                copy().wait_send()

    def apply_operator(h, ref, dst):
        for k in range(planes):
            v = ref[k]
            before = zh[h, 0] if k == 0 else ref[k - 1]
            after = zh[h, 1] if k == last else ref[k + 1]
            beside = before + after
            beside += jnp.where(row_at == 0, xh[h, 0, k:k + 1], pltpu.roll(v, 1, 0))
            beside += jnp.where(row_at == xb - 1, xh[h, 1, k:k + 1], pltpu.roll(v, xb - 1, 0))
            beside += jnp.where(col_at == 0, 0.0, pltpu.roll(v, 1, 1))
            beside += jnp.where(col_at == ny - 1, 0.0, pltpu.roll(v, ny - 1, 1))
            dst[k] = (6.0 + diag_ref[k]) * v - beside

    lane = lax.broadcasted_iota(jnp.int32, (1, ny), 1)

    def summed(pairs):
        row = jnp.zeros((1, ny), F32)
        for i, (a, b) in enumerate(pairs):
            acc = a[0] * b[0]
            for k in range(1, planes):
                acc = acc + a[k] * b[k]
            total = jnp.sum(jnp.sum(acc, axis=0, keepdims=True), axis=1, keepdims=True)
            row = jnp.where(lane == i, total, row)
        return row

    def spread_layer(r, back):
        to = lax.rem(l + r, depth)
        slot = lax.rem(l + depth - r, depth) if back else l
        return pltpu.make_async_remote_copy(
            src_ref=srow, dst_ref=sall.at[slot], send_sem=ls_sem.at[r], recv_sem=lr_sem.at[r],
            device_id=(to, s), device_id_type=MESH)

    def spread_split(r, back):
        slot = s ^ r if back else s
        return pltpu.make_async_remote_copy(
            src_ref=trow, dst_ref=tall.at[slot], send_sem=ts_sem.at[r], recv_sem=tr_sem.at[r],
            device_id=(l, s ^ r), device_id_type=MESH)

    barrier = pltpu.get_barrier_semaphore()
    for r in range(1, parts):
        pl.semaphore_signal(barrier, inc=1, device_id=(l, s ^ r), device_id_type=MESH)
    for r in range(1, depth):
        pl.semaphore_signal(barrier, inc=1, device_id=(lax.rem(l + r, depth), s), device_id_type=MESH)

    def own_copy(k):
        return pltpu.make_async_copy(inv_ref.at[k], mf.at[k, s], own_sem.at[k])

    for k in range(planes):
        own_copy(k).start()
    for k in range(planes):
        turned = jnp.transpose(rs_ref[k])
        for r in range(parts):
            rsend[r, k] = turned[r * yb:(r + 1) * yb]
    stage_lines(0, rs_ref)
    pl.semaphore_wait(barrier, parts + depth - 2)

    def regroup(src, dst, ssem, rsem, r):
        return pltpu.make_async_remote_copy(
            src_ref=src.at[s ^ r], dst_ref=dst.at[s], send_sem=ssem.at[r], recv_sem=rsem.at[r],
            device_id=(l, s ^ r), device_id_type=MESH)

    def regroup_in(src, dst, ssem, rsem, r):
        return pltpu.make_async_remote_copy(
            src_ref=src.at[s ^ r], dst_ref=dst.at[s ^ r], send_sem=ssem.at[r], recv_sem=rsem.at[r],
            device_id=(l, s ^ r), device_id_type=MESH)

    def shift(k, r, b):
        src = inv_ref.at[k] if r == 0 else mf.at[k, s ^ r]
        return pltpu.make_async_remote_copy(
            src_ref=src, dst_ref=mf.at[k, s ^ r], send_sem=gs_sem.at[k, r ^ b], recv_sem=gr_sem.at[k, r ^ b],
            device_id=(l, s ^ b), device_id_type=MESH)

    def arrived(k, r):
        return pltpu.make_async_remote_copy(
            src_ref=mf.at[k, s ^ r], dst_ref=mf.at[k, s ^ r], send_sem=gs_sem.at[k, r], recv_sem=gr_sem.at[k, r],
            device_id=(l, s ^ 1), device_id_type=MESH)

    for r in range(1, parts):
        regroup(rsend, rrecv, as_sem, ar_sem, r).start()
    for k in range(planes):
        for b in reversed(bits):
            shift(k, 0, b).start()
    halo_start(0, rs_ref)
    rrecv[s] = rsend[s]
    for r in range(1, parts):
        regroup_in(rsend, rrecv, as_sem, ar_sem, r).wait_recv()

    def fetch(k):
        for r in range(1, parts):
            arrived(k, r).wait_recv()
            for b in bits:
                if b < (r & -r):
                    shift(k, r, b).start()
        own_copy(k).wait()
        for j in range(parts):
            hi, lo = halves(mf[k, j])
            mhi[k, :, j * xb:(j + 1) * xb] = hi
            mlo[k, :, j * xb:(j + 1) * xb] = lo

    def source(k):
        return jnp.concatenate([rrecv[j, k] for j in range(parts)], axis=1)

    half = nx // 2

    halo_wait(0, rs_ref)
    apply_operator(0, rs_ref, arhs)
    fetch(0)
    for j in range(parts):
        hi, lo = halves(jnp.transpose(mf[0, j]))
        whi[0, j * xb:(j + 1) * xb] = hi
        wlo[0, j * xb:(j + 1) * xb] = lo
    loc[0] = product(*halves(source(0)), mhi[0], mlo[0], 1)

    @pl.loop(1, planes)
    def _(k):
        fetch(k)
        loc[k] = product(*halves(source(k) + loc[k - 1]), mhi[k], mlo[k], 1)
        for t in range(2):
            rows = slice(t * half, (t + 1) * half)
            hi, lo = halves(product(whi[k - 1, rows], wlo[k - 1, rows], mhi[k], mlo[k], 1))
            whi[k, rows] = hi
            wlo[k, rows] = lo

    def hop(src, dst, ssem, rsem, c, step):
        return pltpu.make_async_remote_copy(
            src_ref=src.at[c], dst_ref=dst.at[c], send_sem=ssem.at[c], recv_sem=rsem.at[c],
            device_id=(lax.rem(l + step + depth, depth), s), device_id_type=MESH)

    def down_chain():
        for c in range(chunks):
            rows = slice(c * cb, (c + 1) * cb)

            @pl.when(l > 0)
            def _():
                hop(vout, vin, vs_sem, vr_sem, c, 1).wait_recv()

            @pl.when(l == 0)
            def _():
                vin[c] = jnp.zeros_like(vin[c])

            vout[c] = loc[last, rows] + product(*halves(vin[c]), whi[last], wlo[last], 0)

            @pl.when(l < depth - 1)
            def _():
                hop(vout, vin, vs_sem, vr_sem, c, 1).start()

    def compose():
        for j in range(parts):
            hi, lo = halves(jnp.transpose(mf[last, j]))
            uhi[last, j * xb:(j + 1) * xb] = hi
            ulo[last, j * xb:(j + 1) * xb] = lo

        @pl.loop(0, last)
        def _(i):
            k = last - 1 - i
            loc[k] = loc[k] + product(*halves(loc[k + 1]), mhi[k], mlo[k], 1)
            for t in range(2):
                rows = slice(t * half, (t + 1) * half)
                hi, lo = halves(product(uhi[k + 1, rows], ulo[k + 1, rows], mhi[k], mlo[k], 1))
                uhi[k, rows] = hi
                ulo[k, rows] = lo
                own = whi[k, rows].astype(F32) + wlo[k, rows].astype(F32)
                hi, lo = halves(own + product(whi[k + 1, rows], wlo[k + 1, rows], mhi[k], mlo[k], 1))
                whi[k, rows] = hi
                wlo[k, rows] = lo

    early = lax.convert_element_type(l < depth // 2, jnp.int32)

    @pl.loop(0, 2)
    def _(turn):
        @pl.when(turn != early)
        def _():
            down_chain()

        @pl.when(turn == early)
        def _():
            compose()

    entering = jnp.concatenate([vin[c] for c in range(chunks)], axis=0)
    entering = halves(entering)

    @pl.loop(0, planes)
    def _(k):
        base[k] = loc[k] + product(*entering, whi[k], wlo[k], 0)

    for c in range(chunks):
        rows = slice(c * cb, (c + 1) * cb)

        @pl.when(l < depth - 1)
        def _():
            hop(dout, din, ds_sem, dr_sem, c, -1).wait_recv()

        @pl.when(l == depth - 1)
        def _():
            din[c] = jnp.zeros_like(din[c])

        dout[c] = base[0, rows] + product(*halves(din[c]), uhi[0], ulo[0], 0)

        @pl.when(l > 0)
        def _():
            hop(dout, din, ds_sem, dr_sem, c, -1).start()

    entering = halves(jnp.concatenate([din[c] for c in range(chunks)], axis=0))

    @pl.loop(0, planes)
    def _(k):
        swept = base[k] + product(*entering, uhi[k], ulo[k], 0)
        for j in range(parts):
            dsend[j, k] = swept[:, j * xb:(j + 1) * xb]

    for r in range(1, parts):
        regroup(dsend, drecv, bs_sem, br_sem, r).start()
    drecv[s] = dsend[s]
    for r in range(1, parts):
        regroup_in(dsend, drecv, bs_sem, br_sem, r).wait_recv()
    for k in range(planes):
        dirn[k] = jnp.transpose(jnp.concatenate([drecv[j, k] for j in range(parts)], axis=0))

    stage_lines(1, dirn)
    halo_start(1, dirn)
    halo_wait(1, dirn)
    apply_operator(1, dirn, img)
    stage_lines(2, img)
    halo_start(2, img)
    halo_wait(2, img)
    apply_operator(2, img, aimg)
    srow[...] = summed([
        (rs_ref, rs_ref), (rs_ref, img), (arhs, rs_ref), (arhs, img), (aimg, rs_ref), (aimg, img),
        (arhs, arhs), (arhs, aimg), (aimg, aimg)])
    for r in range(1, depth):
        spread_layer(r, False).start()
    sall[l] = srow[...]
    for r in range(1, depth):
        spread_layer(r, True).wait_recv()
    row = sall[0]
    for i in range(1, depth):
        row = row + sall[i]
    trow[...] = row
    for r in range(1, parts):
        spread_split(r, False).start()
    tall[s] = trow[...]
    for r in range(1, parts):
        spread_split(r, True).wait_recv()
    row = tall[0]
    for i in range(1, parts):
        row = row + tall[i]

    def total(i):
        return jnp.sum(jnp.where(lane == i, row, 0.0), axis=1, keepdims=True)

    alpha = total(0) / total(1)
    cross = total(2) - alpha * (total(3) + total(4)) + alpha * alpha * total(5)
    own = total(6) - 2.0 * alpha * total(7) + alpha * alpha * total(8)
    omega = cross / own
    for k in range(planes):
        middle = rs_ref[k] - alpha * img[k]
        sol_ref[k] = alpha * dirn[k] + omega * middle
        res_ref[k] = middle - omega * (arhs[k] - alpha * aimg[k])

    for h, ref in ((0, rs_ref), (1, dirn), (2, img)):
        halo_finish(h, ref)
    for r in range(1, depth):
        spread_layer(r, False).wait_send()
    for r in range(1, parts):
        spread_split(r, False).wait_send()

    for r in range(1, parts):
        regroup(rsend, rrecv, as_sem, ar_sem, r).wait_send()
        regroup(dsend, drecv, bs_sem, br_sem, r).wait_send()
    for k in range(planes):
        for r in range(1, parts):
            arrived(k, r).wait_send()
    for c in range(chunks):
        @pl.when(l < depth - 1)
        def _():
            hop(vout, vin, vs_sem, vr_sem, c, 1).wait_send()

        @pl.when(l > 0)
        def _():
            hop(dout, din, ds_sem, dr_sem, c, -1).wait_send()


def per_device(right_side, diagonal, inverses):
    depth, parts = lax.axis_size("layer"), lax.axis_size("split")
    planes, nx, xb = inverses.shape
    ny = right_side.shape[2]
    yb = ny // parts
    chunks = 2 if yb % 16 == 0 else 1
    square = pltpu.VMEM((planes, nx, nx), BF16)
    lines = pltpu.VMEM((planes, yb, nx), F32)
    pieces = pltpu.VMEM((parts, planes, yb, xb), F32)
    carry = pltpu.VMEM((chunks, yb // chunks, nx), F32)
    dma = pltpu.SemaphoreType.DMA
    field = pltpu.VMEM(right_side.shape, F32)
    plane = right_side.shape[1:]
    return pl.pallas_call(
        functools.partial(sweep_kernel, depth, parts),
        out_shape=[jax.ShapeDtypeStruct(right_side.shape, F32)] * 2,
        in_specs=[pl.BlockSpec(memory_space=pltpu.VMEM)] * 3,
        out_specs=[pl.BlockSpec(memory_space=pltpu.VMEM)] * 2,
        scratch_shapes=[
            pltpu.VMEM((planes, parts, nx, xb), F32),
            square, square, square, square, square, square,
            lines, lines, pieces, pieces, carry, carry, carry, carry, pieces, pieces,
            field, field, field, field,
            pltpu.VMEM((3, 2) + plane, F32), pltpu.VMEM((3, 2, planes, ny), F32), pltpu.VMEM((3, 2, planes, ny), F32),
            pltpu.VMEM((1, ny), F32), pltpu.VMEM((depth, 1, ny), F32),
            pltpu.VMEM((1, ny), F32), pltpu.VMEM((parts, 1, ny), F32),
            dma((3, 4)), dma((3, 4)), dma((depth,)), dma((depth,)), dma((parts,)), dma((parts,)),
            dma((planes,)), dma((planes, parts)), dma((planes, parts)),
            dma((parts,)), dma((parts,)), dma((parts,)), dma((parts,)),
            dma((chunks,)), dma((chunks,)), dma((chunks,)), dma((chunks,)),
        ],
        compiler_params=pltpu.CompilerParams(
            collective_id=0, has_side_effects=True, vmem_limit_bytes=60 * 1024 * 1024),
    )(right_side, diagonal, inverses)


def solution(mesh):
    placed = (P("layer", "split", None), P("layer", "split", None), P("layer", None, "split"))
    return jax.shard_map(
        per_device,
        mesh=mesh,
        in_specs=placed,
        out_specs=(P("layer", "split", None), P("layer", "split", None)),
        check_vma=False,
    )
```

```python
import functools

import jax
import jax.numpy as jnp
from jax import lax
from jax.experimental import pallas as pl
from jax.experimental.pallas import tpu as pltpu
from jax.sharding import PartitionSpec as P

MESH = pl.DeviceIdType.MESH
F32, BF16 = jnp.float32, jnp.bfloat16


def halves(a):
    hi = a.astype(BF16)
    return hi, (a - hi.astype(F32)).astype(BF16)


def product(a_hi, a_lo, b_hi, b_lo, axis):
    dims = (((1,), (axis,)), ((), ()))

    def one(a, b):
        return lax.dot_general(a, b, dims, preferred_element_type=F32)

    return one(a_hi, b_hi) + (one(a_lo, b_hi) + one(a_hi, b_lo))


def sweep_kernel(
    depth, parts, rs_ref, diag_ref, inv_ref, sol_ref, res_ref,
    mf, mhi, mlo, whi, wlo, uhi, ulo, loc, base, rsend, rrecv, vin, vout, din, dout, dsend, drecv,
    arhs, dirn, img, aimg, zh, xh, xs, srow, sall, trow, tall,
    hs_sem, hr_sem, ls_sem, lr_sem, ts_sem, tr_sem,
    own_sem, gs_sem, gr_sem, as_sem, ar_sem, bs_sem, br_sem, vs_sem, vr_sem, ds_sem, dr_sem,
):
    planes, nx, xb = inv_ref.shape
    ny = rs_ref.shape[2]
    yb = ny // parts
    chunks = vin.shape[0]
    cb = yb // chunks
    l, s = lax.axis_index("layer"), lax.axis_index("split")
    bits = [1 << i for i in range(parts.bit_length() - 1)]

    last = planes - 1
    row_at = lax.broadcasted_iota(jnp.int32, (xb, ny), 0)
    col_at = lax.broadcasted_iota(jnp.int32, (xb, ny), 1)

    def stage_lines(h, ref):
        for k in range(planes):
            xs[h, 0, k:k + 1] = ref[k, 0:1]
            xs[h, 1, k:k + 1] = ref[k, xb - 1:xb]

    def halo_copies(h, ref):
        def zcopy(side, slot):
            return pltpu.make_async_remote_copy(
                src_ref=ref.at[0 if side == 0 else last], dst_ref=zh.at[h, slot], send_sem=hs_sem.at[h, side],
                recv_sem=hr_sem.at[h, slot],
                device_id=(lax.rem(l + 2 * side - 1 + depth, depth), s), device_id_type=MESH)

        def xcopy(side, slot):
            return pltpu.make_async_remote_copy(
                src_ref=xs.at[h, side], dst_ref=xh.at[h, slot], send_sem=hs_sem.at[h, 2 + side],
                recv_sem=hr_sem.at[h, 2 + slot],
                device_id=(l, lax.rem(s + 2 * side - 1 + parts, parts)), device_id_type=MESH)

        out = []
        for side in range(2):
            zhas = l > 0 if side == 0 else l < depth - 1
            xhas = s > 0 if side == 0 else s < parts - 1
            for has, copy, slot in ((zhas, zcopy, zh), (xhas, xcopy, xh)):
                out.append((
                    has, functools.partial(copy, side, 1 - side), functools.partial(copy, side, side),
                    slot.at[h, side]))
        return out

    def halo_start(h, ref):
        for has, copy, _, _ in halo_copies(h, ref):
            @pl.when(has)
            def _():
                copy().start()

    def halo_wait(h, ref):
        for has, _, back, slot in halo_copies(h, ref):
            @pl.when(has)
            def _():
                back().wait_recv()

            @pl.when(jnp.logical_not(has))
            def _():
                slot[...] = jnp.zeros_like(slot[...])

    def halo_finish(h, ref):
        for has, copy, _, _ in halo_copies(h, ref):
            @pl.when(has)
            def _():
                copy().wait_send()

    def apply_operator(h, ref, dst):
        for k in range(planes):
            v = ref[k]
            before = zh[h, 0] if k == 0 else ref[k - 1]
            after = zh[h, 1] if k == last else ref[k + 1]
            beside = before + after
            beside += jnp.where(row_at == 0, xh[h, 0, k:k + 1], pltpu.roll(v, 1, 0))
            beside += jnp.where(row_at == xb - 1, xh[h, 1, k:k + 1], pltpu.roll(v, xb - 1, 0))
            beside += jnp.where(col_at == 0, 0.0, pltpu.roll(v, 1, 1))
            beside += jnp.where(col_at == ny - 1, 0.0, pltpu.roll(v, ny - 1, 1))
            dst[k] = (6.0 + diag_ref[k]) * v - beside

    lane = lax.broadcasted_iota(jnp.int32, (1, ny), 1)

    def summed(pairs):
        row = jnp.zeros((1, ny), F32)
        for i, (a, b) in enumerate(pairs):
            acc = a[0] * b[0]
            for k in range(1, planes):
                acc = acc + a[k] * b[k]
            total = jnp.sum(jnp.sum(acc, axis=0, keepdims=True), axis=1, keepdims=True)
            row = jnp.where(lane == i, total, row)
        return row

    def spread_layer(r, back):
        to = lax.rem(l + r, depth)
        slot = lax.rem(l + depth - r, depth) if back else l
        return pltpu.make_async_remote_copy(
            src_ref=srow, dst_ref=sall.at[slot], send_sem=ls_sem.at[r], recv_sem=lr_sem.at[r],
            device_id=(to, s), device_id_type=MESH)

    def spread_split(r, back):
        slot = s ^ r if back else s
        return pltpu.make_async_remote_copy(
            src_ref=trow, dst_ref=tall.at[slot], send_sem=ts_sem.at[r], recv_sem=tr_sem.at[r],
            device_id=(l, s ^ r), device_id_type=MESH)

    barrier = pltpu.get_barrier_semaphore()
    for r in range(1, parts):
        pl.semaphore_signal(barrier, inc=1, device_id=(l, s ^ r), device_id_type=MESH)
    for r in range(1, depth):
        pl.semaphore_signal(barrier, inc=1, device_id=(lax.rem(l + r, depth), s), device_id_type=MESH)

    def own_copy(k):
        return pltpu.make_async_copy(inv_ref.at[k], mf.at[k, s], own_sem.at[k])

    for k in range(planes):
        own_copy(k).start()
    for k in range(planes):
        turned = jnp.transpose(rs_ref[k])
        for r in range(parts):
            rsend[r, k] = turned[r * yb:(r + 1) * yb]
    stage_lines(0, rs_ref)
    pl.semaphore_wait(barrier, parts + depth - 2)

    def regroup(src, dst, ssem, rsem, r):
        return pltpu.make_async_remote_copy(
            src_ref=src.at[s ^ r], dst_ref=dst.at[s], send_sem=ssem.at[r], recv_sem=rsem.at[r],
            device_id=(l, s ^ r), device_id_type=MESH)

    def regroup_in(src, dst, ssem, rsem, r):
        return pltpu.make_async_remote_copy(
            src_ref=src.at[s ^ r], dst_ref=dst.at[s ^ r], send_sem=ssem.at[r], recv_sem=rsem.at[r],
            device_id=(l, s ^ r), device_id_type=MESH)

    cuts = 2
    cut = nx // cuts

    def shift(k, h, r, b):
        rows = pl.ds(h * cut, cut)
        src = inv_ref.at[k, rows] if r == 0 else mf.at[k, s ^ r, rows]
        return pltpu.make_async_remote_copy(
            src_ref=src, dst_ref=mf.at[k, s ^ r, rows],
            send_sem=gs_sem.at[k * cuts + h, r ^ b], recv_sem=gr_sem.at[k * cuts + h, r ^ b],
            device_id=(l, s ^ b), device_id_type=MESH)

    def arrived(k, h, r):
        rows = pl.ds(h * cut, cut)
        return pltpu.make_async_remote_copy(
            src_ref=mf.at[k, s ^ r, rows], dst_ref=mf.at[k, s ^ r, rows],
            send_sem=gs_sem.at[k * cuts + h, r], recv_sem=gr_sem.at[k * cuts + h, r],
            device_id=(l, s ^ 1), device_id_type=MESH)

    for r in range(1, parts):
        regroup(rsend, rrecv, as_sem, ar_sem, r).start()
    halo_start(0, rs_ref)
    for h in range(cuts):
        for b in reversed(bits):
            shift(0, h, 0, b).start()
    rrecv[s] = rsend[s]
    for r in range(1, parts):
        regroup_in(rsend, rrecv, as_sem, ar_sem, r).wait_recv()

    def fetch(k):
        for h in range(cuts):
            for r in range(1, parts):
                arrived(k, h, r).wait_recv()
                for b in bits:
                    if b < (r & -r):
                        shift(k, h, r, b).start()
                if r == bits[-1]:
                    @pl.when(k < last)
                    def _():
                        for b in reversed(bits):
                            shift(k + 1, h, 0, b).start()
        own_copy(k).wait()
        for j in range(parts):
            hi, lo = halves(mf[k, j])
            mhi[k, :, j * xb:(j + 1) * xb] = hi
            mlo[k, :, j * xb:(j + 1) * xb] = lo

    def source(k):
        return jnp.concatenate([rrecv[j, k] for j in range(parts)], axis=1)

    half = nx // 2

    def hop(src, dst, ssem, rsem, c, step):
        return pltpu.make_async_remote_copy(
            src_ref=src.at[c], dst_ref=dst.at[c], send_sem=ssem.at[c], recv_sem=rsem.at[c],
            device_id=(lax.rem(l + step + depth, depth), s), device_id_type=MESH)

    fetch(0)
    for j in range(parts):
        hi, lo = halves(jnp.transpose(mf[0, j]))
        whi[0, j * xb:(j + 1) * xb] = hi
        wlo[0, j * xb:(j + 1) * xb] = lo
    loc[0] = product(*halves(source(0)), mhi[0], mlo[0], 1)

    halo_wait(0, rs_ref)
    apply_operator(0, rs_ref, arhs)

    @pl.loop(1, planes)
    def _(k):
        fetch(k)
        loc[k] = product(*halves(source(k) + loc[k - 1]), mhi[k], mlo[k], 1)

        @pl.when(jnp.logical_and(k == last, l == 0))
        def _():
            for c in range(chunks):
                vin[c] = jnp.zeros_like(vin[c])
                vout[c] = loc[last, c * cb:(c + 1) * cb]
            for c in range(chunks):
                hop(vout, vin, vs_sem, vr_sem, c, 1).start()

        for t in range(2):
            rows = slice(t * half, (t + 1) * half)
            hi, lo = halves(product(whi[k - 1, rows], wlo[k - 1, rows], mhi[k], mlo[k], 1))
            whi[k, rows] = hi
            wlo[k, rows] = lo

    def down_chain():
        for c in range(chunks):
            rows = slice(c * cb, (c + 1) * cb)
            hop(vout, vin, vs_sem, vr_sem, c, 1).wait_recv()
            vout[c] = loc[last, rows] + product(*halves(vin[c]), whi[last], wlo[last], 0)

            @pl.when(l < depth - 1)
            def _():
                hop(vout, vin, vs_sem, vr_sem, c, 1).start()

    def compose():
        for j in range(parts):
            hi, lo = halves(jnp.transpose(mf[last, j]))
            uhi[last, j * xb:(j + 1) * xb] = hi
            ulo[last, j * xb:(j + 1) * xb] = lo

        @pl.loop(0, last)
        def _(i):
            k = last - 1 - i
            loc[k] = loc[k] + product(*halves(loc[k + 1]), mhi[k], mlo[k], 1)
            for t in range(2):
                rows = slice(t * half, (t + 1) * half)
                hi, lo = halves(product(uhi[k + 1, rows], ulo[k + 1, rows], mhi[k], mlo[k], 1))
                uhi[k, rows] = hi
                ulo[k, rows] = lo
                own = whi[k, rows].astype(F32) + wlo[k, rows].astype(F32)
                hi, lo = halves(own + product(whi[k + 1, rows], wlo[k + 1, rows], mhi[k], mlo[k], 1))
                whi[k, rows] = hi
                wlo[k, rows] = lo

    early = lax.convert_element_type(l < depth // 2, jnp.int32)

    @pl.loop(0, 2)
    def _(turn):
        @pl.when(jnp.logical_and(turn != early, l > 0))
        def _():
            down_chain()

        @pl.when(turn == early)
        def _():
            compose()

    entering = jnp.concatenate([vin[c] for c in range(chunks)], axis=0)
    entering = halves(entering)

    @pl.loop(0, planes)
    def _(k):
        base[k] = loc[k] + product(*entering, whi[k], wlo[k], 0)

    for c in range(chunks):
        rows = slice(c * cb, (c + 1) * cb)

        @pl.when(l < depth - 1)
        def _():
            hop(dout, din, ds_sem, dr_sem, c, -1).wait_recv()

        @pl.when(l == depth - 1)
        def _():
            din[c] = jnp.zeros_like(din[c])

        dout[c] = base[0, rows] + product(*halves(din[c]), uhi[0], ulo[0], 0)

        @pl.when(l > 0)
        def _():
            hop(dout, din, ds_sem, dr_sem, c, -1).start()

    entering = halves(jnp.concatenate([din[c] for c in range(chunks)], axis=0))

    @pl.loop(0, planes)
    def _(k):
        swept = base[k] + product(*entering, uhi[k], ulo[k], 0)
        for j in range(parts):
            dsend[j, k] = swept[:, j * xb:(j + 1) * xb]

    for r in range(1, parts):
        regroup(dsend, drecv, bs_sem, br_sem, r).start()
    drecv[s] = dsend[s]
    for r in range(1, parts):
        regroup_in(dsend, drecv, bs_sem, br_sem, r).wait_recv()
    for k in range(planes):
        dirn[k] = jnp.transpose(jnp.concatenate([drecv[j, k] for j in range(parts)], axis=0))

    stage_lines(1, dirn)
    halo_start(1, dirn)
    halo_wait(1, dirn)
    apply_operator(1, dirn, img)
    stage_lines(2, img)
    halo_start(2, img)
    halo_wait(2, img)
    apply_operator(2, img, aimg)
    srow[...] = summed([
        (rs_ref, rs_ref), (rs_ref, img), (arhs, rs_ref), (arhs, img), (aimg, rs_ref), (aimg, img),
        (arhs, arhs), (arhs, aimg), (aimg, aimg)])
    for r in range(1, depth):
        spread_layer(r, False).start()
    sall[l] = srow[...]
    for r in range(1, depth):
        spread_layer(r, True).wait_recv()
    row = sall[0]
    for i in range(1, depth):
        row = row + sall[i]
    trow[...] = row
    for r in range(1, parts):
        spread_split(r, False).start()
    tall[s] = trow[...]
    for r in range(1, parts):
        spread_split(r, True).wait_recv()
    row = tall[0]
    for i in range(1, parts):
        row = row + tall[i]

    def total(i):
        return jnp.sum(jnp.where(lane == i, row, 0.0), axis=1, keepdims=True)

    alpha = total(0) / total(1)
    cross = total(2) - alpha * (total(3) + total(4)) + alpha * alpha * total(5)
    own = total(6) - 2.0 * alpha * total(7) + alpha * alpha * total(8)
    omega = cross / own
    for k in range(planes):
        middle = rs_ref[k] - alpha * img[k]
        sol_ref[k] = alpha * dirn[k] + omega * middle
        res_ref[k] = middle - omega * (arhs[k] - alpha * aimg[k])

    for h, ref in ((0, rs_ref), (1, dirn), (2, img)):
        halo_finish(h, ref)
    for r in range(1, depth):
        spread_layer(r, False).wait_send()
    for r in range(1, parts):
        spread_split(r, False).wait_send()

    for r in range(1, parts):
        regroup(rsend, rrecv, as_sem, ar_sem, r).wait_send()
        regroup(dsend, drecv, bs_sem, br_sem, r).wait_send()
    for k in range(planes):
        for r in range(1, parts):
            for h in range(cuts):
                arrived(k, h, r).wait_send()
    for c in range(chunks):
        @pl.when(l < depth - 1)
        def _():
            hop(vout, vin, vs_sem, vr_sem, c, 1).wait_send()

        @pl.when(l > 0)
        def _():
            hop(dout, din, ds_sem, dr_sem, c, -1).wait_send()


def per_device(right_side, diagonal, inverses):
    depth, parts = lax.axis_size("layer"), lax.axis_size("split")
    planes, nx, xb = inverses.shape
    ny = right_side.shape[2]
    yb = ny // parts
    chunks = yb // 8 if yb % 8 == 0 else 1
    square = pltpu.VMEM((planes, nx, nx), BF16)
    lines = pltpu.VMEM((planes, yb, nx), F32)
    pieces = pltpu.VMEM((parts, planes, yb, xb), F32)
    carry = pltpu.VMEM((chunks, yb // chunks, nx), F32)
    dma = pltpu.SemaphoreType.DMA
    field = pltpu.VMEM(right_side.shape, F32)
    plane = right_side.shape[1:]
    return pl.pallas_call(
        functools.partial(sweep_kernel, depth, parts),
        out_shape=[jax.ShapeDtypeStruct(right_side.shape, F32)] * 2,
        in_specs=[pl.BlockSpec(memory_space=pltpu.VMEM)] * 3,
        out_specs=[pl.BlockSpec(memory_space=pltpu.VMEM)] * 2,
        scratch_shapes=[
            pltpu.VMEM((planes, parts, nx, xb), F32),
            square, square, square, square, square, square,
            lines, lines, pieces, pieces, carry, carry, carry, carry, pieces, pieces,
            field, field, field, field,
            pltpu.VMEM((3, 2) + plane, F32), pltpu.VMEM((3, 2, planes, ny), F32), pltpu.VMEM((3, 2, planes, ny), F32),
            pltpu.VMEM((1, ny), F32), pltpu.VMEM((depth, 1, ny), F32),
            pltpu.VMEM((1, ny), F32), pltpu.VMEM((parts, 1, ny), F32),
            dma((3, 4)), dma((3, 4)), dma((depth,)), dma((depth,)), dma((parts,)), dma((parts,)),
            dma((planes,)), dma((planes * 2, parts)), dma((planes * 2, parts)),
            dma((parts,)), dma((parts,)), dma((parts,)), dma((parts,)),
            dma((chunks,)), dma((chunks,)), dma((chunks,)), dma((chunks,)),
        ],
        compiler_params=pltpu.CompilerParams(
            collective_id=0, has_side_effects=True, vmem_limit_bytes=60 * 1024 * 1024),
    )(right_side, diagonal, inverses)


def solution(mesh):
    placed = (P("layer", "split", None), P("layer", "split", None), P("layer", None, "split"))
    return jax.shard_map(
        per_device,
        mesh=mesh,
        in_specs=placed,
        out_specs=(P("layer", "split", None), P("layer", "split", None)),
        check_vma=False,
    )
```

```python
import functools

import jax
import jax.numpy as jnp
from jax import lax
from jax.experimental import pallas as pl
from jax.experimental.pallas import tpu as pltpu
from jax.sharding import PartitionSpec as P

MESH = pl.DeviceIdType.MESH
F32, BF16 = jnp.float32, jnp.bfloat16


def halves(a):
    hi = a.astype(BF16)
    return hi, (a - hi.astype(F32)).astype(BF16)


def product(a_hi, a_lo, b_hi, b_lo, axis):
    dims = (((1,), (axis,)), ((), ()))

    def one(a, b):
        return lax.dot_general(a, b, dims, preferred_element_type=F32)

    return one(a_hi, b_hi) + (one(a_lo, b_hi) + one(a_hi, b_lo))


def sweep_kernel(
    depth, parts, rs_ref, diag_ref, inv_ref, sol_ref, res_ref,
    mf, mhi, mlo, whi, wlo, uhi, ulo, loc, base, rsend, rrecv, vin, vout, din, dout, dsend, drecv,
    usend, uland, phi, plo, vhi, vlo, bodd, cst, pin, us_sem, ur_sem, bo_s, bo_r, ps_sem, pr_sem,
    arhs, dirn, img, aimg, zh, xh, xs, srow, sall, trow, tall,
    hs_sem, hr_sem, ls_sem, lr_sem, ts_sem, tr_sem,
    own_sem, gs_sem, gr_sem, as_sem, ar_sem, bs_sem, br_sem, vs_sem, vr_sem, ds_sem, dr_sem,
):
    planes, nx, xb = inv_ref.shape
    ny = rs_ref.shape[2]
    yb = ny // parts
    chunks = vin.shape[0]
    cb = yb // chunks
    l, s = lax.axis_index("layer"), lax.axis_index("split")
    bits = [1 << i for i in range(parts.bit_length() - 1)]

    last = planes - 1
    row_at = lax.broadcasted_iota(jnp.int32, (xb, ny), 0)
    col_at = lax.broadcasted_iota(jnp.int32, (xb, ny), 1)

    def stage_lines(h, ref):
        for k in range(planes):
            xs[h, 0, k:k + 1] = ref[k, 0:1]
            xs[h, 1, k:k + 1] = ref[k, xb - 1:xb]

    def halo_copies(h, ref):
        def zcopy(side, slot):
            return pltpu.make_async_remote_copy(
                src_ref=ref.at[0 if side == 0 else last], dst_ref=zh.at[h, slot], send_sem=hs_sem.at[h, side],
                recv_sem=hr_sem.at[h, slot],
                device_id=(lax.rem(l + 2 * side - 1 + depth, depth), s), device_id_type=MESH)

        def xcopy(side, slot):
            return pltpu.make_async_remote_copy(
                src_ref=xs.at[h, side], dst_ref=xh.at[h, slot], send_sem=hs_sem.at[h, 2 + side],
                recv_sem=hr_sem.at[h, 2 + slot],
                device_id=(l, lax.rem(s + 2 * side - 1 + parts, parts)), device_id_type=MESH)

        out = []
        for side in range(2):
            zhas = l > 0 if side == 0 else l < depth - 1
            xhas = s > 0 if side == 0 else s < parts - 1
            for has, copy, slot in ((zhas, zcopy, zh), (xhas, xcopy, xh)):
                out.append((
                    has, functools.partial(copy, side, 1 - side), functools.partial(copy, side, side),
                    slot.at[h, side]))
        return out

    def halo_start(h, ref):
        for has, copy, _, _ in halo_copies(h, ref):
            @pl.when(has)
            def _():
                copy().start()

    def halo_wait(h, ref):
        for has, _, back, slot in halo_copies(h, ref):
            @pl.when(has)
            def _():
                back().wait_recv()

            @pl.when(jnp.logical_not(has))
            def _():
                slot[...] = jnp.zeros_like(slot[...])

    def halo_finish(h, ref):
        for has, copy, _, _ in halo_copies(h, ref):
            @pl.when(has)
            def _():
                copy().wait_send()

    def apply_operator(h, ref, dst):
        for k in range(planes):
            v = ref[k]
            before = zh[h, 0] if k == 0 else ref[k - 1]
            after = zh[h, 1] if k == last else ref[k + 1]
            beside = before + after
            beside += jnp.where(row_at == 0, xh[h, 0, k:k + 1], pltpu.roll(v, 1, 0))
            beside += jnp.where(row_at == xb - 1, xh[h, 1, k:k + 1], pltpu.roll(v, xb - 1, 0))
            beside += jnp.where(col_at == 0, 0.0, pltpu.roll(v, 1, 1))
            beside += jnp.where(col_at == ny - 1, 0.0, pltpu.roll(v, ny - 1, 1))
            dst[k] = (6.0 + diag_ref[k]) * v - beside

    lane = lax.broadcasted_iota(jnp.int32, (1, ny), 1)

    def summed(pairs):
        row = jnp.zeros((1, ny), F32)
        for i, (a, b) in enumerate(pairs):
            acc = a[0] * b[0]
            for k in range(1, planes):
                acc = acc + a[k] * b[k]
            total = jnp.sum(jnp.sum(acc, axis=0, keepdims=True), axis=1, keepdims=True)
            row = jnp.where(lane == i, total, row)
        return row

    def spread_layer(r, back):
        to = lax.rem(l + r, depth)
        slot = lax.rem(l + depth - r, depth) if back else l
        return pltpu.make_async_remote_copy(
            src_ref=srow, dst_ref=sall.at[slot], send_sem=ls_sem.at[r], recv_sem=lr_sem.at[r],
            device_id=(to, s), device_id_type=MESH)

    def spread_split(r, back):
        slot = s ^ r if back else s
        return pltpu.make_async_remote_copy(
            src_ref=trow, dst_ref=tall.at[slot], send_sem=ts_sem.at[r], recv_sem=tr_sem.at[r],
            device_id=(l, s ^ r), device_id_type=MESH)

    barrier = pltpu.get_barrier_semaphore()
    for r in range(1, parts):
        pl.semaphore_signal(barrier, inc=1, device_id=(l, s ^ r), device_id_type=MESH)
    for r in range(1, depth):
        pl.semaphore_signal(barrier, inc=1, device_id=(lax.rem(l + r, depth), s), device_id_type=MESH)

    def own_copy(k):
        return pltpu.make_async_copy(inv_ref.at[k], mf.at[k, s], own_sem.at[k])

    for k in range(planes):
        own_copy(k).start()
    for k in range(planes):
        turned = jnp.transpose(rs_ref[k])
        for r in range(parts):
            rsend[r, k] = turned[r * yb:(r + 1) * yb]
    stage_lines(0, rs_ref)
    pl.semaphore_wait(barrier, parts + depth - 2)

    def regroup(src, dst, ssem, rsem, r):
        return pltpu.make_async_remote_copy(
            src_ref=src.at[s ^ r], dst_ref=dst.at[s], send_sem=ssem.at[r], recv_sem=rsem.at[r],
            device_id=(l, s ^ r), device_id_type=MESH)

    def regroup_in(src, dst, ssem, rsem, r):
        return pltpu.make_async_remote_copy(
            src_ref=src.at[s ^ r], dst_ref=dst.at[s ^ r], send_sem=ssem.at[r], recv_sem=rsem.at[r],
            device_id=(l, s ^ r), device_id_type=MESH)

    cuts = 2
    cut = nx // cuts

    def shift(k, h, r, b):
        rows = pl.ds(h * cut, cut)
        src = inv_ref.at[k, rows] if r == 0 else mf.at[k, s ^ r, rows]
        return pltpu.make_async_remote_copy(
            src_ref=src, dst_ref=mf.at[k, s ^ r, rows],
            send_sem=gs_sem.at[k * cuts + h, r ^ b], recv_sem=gr_sem.at[k * cuts + h, r ^ b],
            device_id=(l, s ^ b), device_id_type=MESH)

    def arrived(k, h, r):
        rows = pl.ds(h * cut, cut)
        return pltpu.make_async_remote_copy(
            src_ref=mf.at[k, s ^ r, rows], dst_ref=mf.at[k, s ^ r, rows],
            send_sem=gs_sem.at[k * cuts + h, r], recv_sem=gr_sem.at[k * cuts + h, r],
            device_id=(l, s ^ 1), device_id_type=MESH)

    for r in range(1, parts):
        regroup(rsend, rrecv, as_sem, ar_sem, r).start()
    halo_start(0, rs_ref)
    for h in range(cuts):
        for b in reversed(bits):
            shift(0, h, 0, b).start()
    rrecv[s] = rsend[s]
    for r in range(1, parts):
        regroup_in(rsend, rrecv, as_sem, ar_sem, r).wait_recv()

    def fetch(k):
        for h in range(cuts):
            for r in range(1, parts):
                arrived(k, h, r).wait_recv()
                for b in bits:
                    if b < (r & -r):
                        shift(k, h, r, b).start()
                if r == bits[-1]:
                    @pl.when(k < last)
                    def _():
                        for b in reversed(bits):
                            shift(k + 1, h, 0, b).start()
        own_copy(k).wait()
        for j in range(parts):
            hi, lo = halves(mf[k, j])
            mhi[k, :, j * xb:(j + 1) * xb] = hi
            mlo[k, :, j * xb:(j + 1) * xb] = lo

    def source(k):
        return jnp.concatenate([rrecv[j, k] for j in range(parts)], axis=1)

    half = nx // 2

    def hop(src, dst, ssem, rsem, c, step):
        return pltpu.make_async_remote_copy(
            src_ref=src.at[c], dst_ref=dst.at[c], send_sem=ssem.at[c], recv_sem=rsem.at[c],
            device_id=(lax.rem(l + step + depth, depth), s), device_id_type=MESH)

    fetch(0)
    for j in range(parts):
        hi, lo = halves(jnp.transpose(mf[0, j]))
        whi[0, j * xb:(j + 1) * xb] = hi
        wlo[0, j * xb:(j + 1) * xb] = lo
    loc[0] = product(*halves(source(0)), mhi[0], mlo[0], 1)

    halo_wait(0, rs_ref)
    apply_operator(0, rs_ref, arhs)

    @pl.loop(1, planes)
    def _(k):
        fetch(k)
        loc[k] = product(*halves(source(k) + loc[k - 1]), mhi[k], mlo[k], 1)

        @pl.when(jnp.logical_and(k == last, l == 0))
        def _():
            for c in range(chunks):
                vin[c] = jnp.zeros_like(vin[c])
                vout[c] = loc[last, c * cb:(c + 1) * cb]
            for c in range(chunks):
                hop(vout, vin, vs_sem, vr_sem, c, 1).start()

        for t in range(2):
            rows = slice(t * half, (t + 1) * half)
            hi, lo = halves(product(whi[k - 1, rows], wlo[k - 1, rows], mhi[k], mlo[k], 1))
            whi[k, rows] = hi
            wlo[k, rows] = lo

    def down_chain():
        for c in range(chunks):
            rows = slice(c * cb, (c + 1) * cb)
            hop(vout, vin, vs_sem, vr_sem, c, 1).wait_recv()
            vout[c] = loc[last, rows] + product(*halves(vin[c]), whi[last], wlo[last], 0)

            @pl.when(l < depth - 1)
            def _():
                hop(vout, vin, vs_sem, vr_sem, c, 1).start()

    odd = l % 2 == 1
    even = jnp.logical_not(odd)
    mine = pl.ds((s % 2) * half, half)
    other = pl.ds((1 - s % 2) * half, half)

    def pair_map():
        return pltpu.make_async_remote_copy(
            src_ref=usend.at[mine], dst_ref=uland.at[mine], send_sem=us_sem.at[0], recv_sem=ur_sem.at[0],
            device_id=(l ^ 1, s), device_id_type=MESH)

    def mate_map(rows):
        return pltpu.make_async_remote_copy(
            src_ref=uland.at[rows], dst_ref=uland.at[rows], send_sem=us_sem.at[1], recv_sem=ur_sem.at[1],
            device_id=(l, s ^ 1), device_id_type=MESH)

    def pair_base():
        return pltpu.make_async_remote_copy(
            src_ref=base.at[0], dst_ref=bodd, send_sem=bo_s.at[0], recv_sem=bo_r.at[0],
            device_id=(l ^ 1, s), device_id_type=MESH)

    def compose():
        for j in range(parts):
            hi, lo = halves(jnp.transpose(mf[last, j]))
            uhi[last, j * xb:(j + 1) * xb] = hi
            ulo[last, j * xb:(j + 1) * xb] = lo

        @pl.loop(0, last)
        def _(i):
            k = last - 1 - i
            loc[k] = loc[k] + product(*halves(loc[k + 1]), mhi[k], mlo[k], 1)
            for t in range(2):
                rows = slice(t * half, (t + 1) * half)
                hi, lo = halves(product(uhi[k + 1, rows], ulo[k + 1, rows], mhi[k], mlo[k], 1))
                uhi[k, rows] = hi
                ulo[k, rows] = lo
                own = whi[k, rows].astype(F32) + wlo[k, rows].astype(F32)
                hi, lo = halves(own + product(whi[k + 1, rows], wlo[k + 1, rows], mhi[k], mlo[k], 1))
                whi[k, rows] = hi
                wlo[k, rows] = lo

        @pl.when(odd)
        def _():
            usend[...] = uhi[0].astype(F32) + ulo[0].astype(F32)
            pair_map().start()

    early = lax.convert_element_type(l < depth // 2, jnp.int32)

    @pl.loop(0, 2)
    def _(turn):
        @pl.when(jnp.logical_and(turn != early, l > 0))
        def _():
            down_chain()

        @pl.when(turn == early)
        def _():
            compose()

    entering = jnp.concatenate([vin[c] for c in range(chunks)], axis=0)
    entering = halves(entering)

    @pl.loop(0, planes)
    def _(k):
        base[k] = loc[k] + product(*entering, whi[k], wlo[k], 0)

        @pl.when(jnp.logical_and(k == 0, odd))
        def _():
            pair_base().start()


    @pl.when(odd)
    def _():
        for c in range(chunks):
            @pl.when(l < depth - 1)
            def _():
                hop(dout, din, ds_sem, dr_sem, c, -1).wait_recv()

            @pl.when(l == depth - 1)
            def _():
                din[c] = jnp.zeros_like(din[c])

    @pl.when(even)
    def _():
        pair_map().wait_recv()
        mate_map(mine).start()
        mate_map(other).wait_recv()
        for i in range(2):
            rows = slice(i * half, (i + 1) * half)
            hi, lo = halves(uland[rows])
            phi[rows] = hi
            plo[rows] = lo

            @pl.when(l > 0)
            def _():
                hi, lo = halves(product(phi[rows], plo[rows], uhi[0], ulo[0], 0))
                vhi[rows] = hi
                vlo[rows] = lo

        pair_base().wait_recv()
        cst[...] = base[0] + product(*halves(bodd[...]), uhi[0], ulo[0], 0)
        for c in range(chunks):
            @pl.when(l < depth - 2)
            def _():
                hop(dout, pin, ps_sem, pr_sem, c, -2).wait_recv()

            @pl.when(l >= depth - 2)
            def _():
                pin[c] = jnp.zeros_like(pin[c])

            @pl.when(l > 0)
            def _():
                rows = slice(c * cb, (c + 1) * cb)
                dout[c] = cst[rows] + product(*halves(pin[c]), vhi[...], vlo[...], 0)
                hop(dout, pin, ps_sem, pr_sem, c, -2).start()
                hop(dout, din, ds_sem, dr_sem, c, -1).start()

        held = bodd[...] + product(
            *halves(jnp.concatenate([pin[c] for c in range(chunks)], axis=0)), phi[...], plo[...], 0)
        for c in range(chunks):
            din[c] = held[c * cb:(c + 1) * cb]

    entering = halves(jnp.concatenate([din[c] for c in range(chunks)], axis=0))

    @pl.loop(0, planes)
    def _(k):
        swept = base[k] + product(*entering, uhi[k], ulo[k], 0)
        for j in range(parts):
            dsend[j, k] = swept[:, j * xb:(j + 1) * xb]

    for r in range(1, parts):
        regroup(dsend, drecv, bs_sem, br_sem, r).start()
    drecv[s] = dsend[s]
    for r in range(1, parts):
        regroup_in(dsend, drecv, bs_sem, br_sem, r).wait_recv()
    for k in range(planes):
        dirn[k] = jnp.transpose(jnp.concatenate([drecv[j, k] for j in range(parts)], axis=0))

    stage_lines(1, dirn)
    halo_start(1, dirn)
    halo_wait(1, dirn)
    apply_operator(1, dirn, img)
    stage_lines(2, img)
    halo_start(2, img)
    halo_wait(2, img)
    apply_operator(2, img, aimg)
    srow[...] = summed([
        (rs_ref, rs_ref), (rs_ref, img), (arhs, rs_ref), (arhs, img), (aimg, rs_ref), (aimg, img),
        (arhs, arhs), (arhs, aimg), (aimg, aimg)])
    for r in range(1, depth):
        spread_layer(r, False).start()
    sall[l] = srow[...]
    for r in range(1, depth):
        spread_layer(r, True).wait_recv()
    row = sall[0]
    for i in range(1, depth):
        row = row + sall[i]
    trow[...] = row
    for r in range(1, parts):
        spread_split(r, False).start()
    tall[s] = trow[...]
    for r in range(1, parts):
        spread_split(r, True).wait_recv()
    row = tall[0]
    for i in range(1, parts):
        row = row + tall[i]

    def total(i):
        return jnp.sum(jnp.where(lane == i, row, 0.0), axis=1, keepdims=True)

    alpha = total(0) / total(1)
    cross = total(2) - alpha * (total(3) + total(4)) + alpha * alpha * total(5)
    own = total(6) - 2.0 * alpha * total(7) + alpha * alpha * total(8)
    omega = cross / own
    for k in range(planes):
        middle = rs_ref[k] - alpha * img[k]
        sol_ref[k] = alpha * dirn[k] + omega * middle
        res_ref[k] = middle - omega * (arhs[k] - alpha * aimg[k])

    for h, ref in ((0, rs_ref), (1, dirn), (2, img)):
        halo_finish(h, ref)
    for r in range(1, depth):
        spread_layer(r, False).wait_send()
    for r in range(1, parts):
        spread_split(r, False).wait_send()

    for r in range(1, parts):
        regroup(rsend, rrecv, as_sem, ar_sem, r).wait_send()
        regroup(dsend, drecv, bs_sem, br_sem, r).wait_send()
    for k in range(planes):
        for r in range(1, parts):
            for h in range(cuts):
                arrived(k, h, r).wait_send()
    for c in range(chunks):
        @pl.when(l < depth - 1)
        def _():
            hop(vout, vin, vs_sem, vr_sem, c, 1).wait_send()

        @pl.when(jnp.logical_and(l > 0, even))
        def _():
            hop(dout, pin, ps_sem, pr_sem, c, -2).wait_send()
            hop(dout, din, ds_sem, dr_sem, c, -1).wait_send()

    @pl.when(odd)
    def _():
        pair_map().wait_send()
        pair_base().wait_send()

    @pl.when(even)
    def _():
        mate_map(mine).wait_send()


def per_device(right_side, diagonal, inverses):
    depth, parts = lax.axis_size("layer"), lax.axis_size("split")
    planes, nx, xb = inverses.shape
    ny = right_side.shape[2]
    yb = ny // parts
    chunks = yb // 8 if yb % 8 == 0 else 1
    flat = pltpu.VMEM((nx, nx), BF16)
    square = pltpu.VMEM((planes, nx, nx), BF16)
    lines = pltpu.VMEM((planes, yb, nx), F32)
    pieces = pltpu.VMEM((parts, planes, yb, xb), F32)
    carry = pltpu.VMEM((chunks, yb // chunks, nx), F32)
    dma = pltpu.SemaphoreType.DMA
    field = pltpu.VMEM(right_side.shape, F32)
    plane = right_side.shape[1:]
    return pl.pallas_call(
        functools.partial(sweep_kernel, depth, parts),
        out_shape=[jax.ShapeDtypeStruct(right_side.shape, F32)] * 2,
        in_specs=[pl.BlockSpec(memory_space=pltpu.VMEM)] * 3,
        out_specs=[pl.BlockSpec(memory_space=pltpu.VMEM)] * 2,
        scratch_shapes=[
            pltpu.VMEM((planes, parts, nx, xb), F32),
            square, square, square, square, square, square,
            lines, lines, pieces, pieces, carry, carry, carry, carry, pieces, pieces,
            pltpu.VMEM((nx, nx), F32), pltpu.VMEM((nx, nx), F32), flat, flat, flat, flat,
            pltpu.VMEM((yb, nx), F32), pltpu.VMEM((yb, nx), F32), carry,
            dma((2,)), dma((2,)), dma((1,)), dma((1,)), dma((chunks,)), dma((chunks,)),
            field, field, field, field,
            pltpu.VMEM((3, 2) + plane, F32), pltpu.VMEM((3, 2, planes, ny), F32), pltpu.VMEM((3, 2, planes, ny), F32),
            pltpu.VMEM((1, ny), F32), pltpu.VMEM((depth, 1, ny), F32),
            pltpu.VMEM((1, ny), F32), pltpu.VMEM((parts, 1, ny), F32),
            dma((3, 4)), dma((3, 4)), dma((depth,)), dma((depth,)), dma((parts,)), dma((parts,)),
            dma((planes,)), dma((planes * 2, parts)), dma((planes * 2, parts)),
            dma((parts,)), dma((parts,)), dma((parts,)), dma((parts,)),
            dma((chunks,)), dma((chunks,)), dma((chunks,)), dma((chunks,)),
        ],
        compiler_params=pltpu.CompilerParams(
            collective_id=0, has_side_effects=True, vmem_limit_bytes=60 * 1024 * 1024),
    )(right_side, diagonal, inverses)


def solution(mesh):
    placed = (P("layer", "split", None), P("layer", "split", None), P("layer", None, "split"))
    return jax.shard_map(
        per_device,
        mesh=mesh,
        in_specs=placed,
        out_specs=(P("layer", "split", None), P("layer", "split", None)),
        check_vma=False,
    )
```
